32 devices in a mesh: rep: 4 (over y, x), shard: 8 (over z, core).
Axes of the slice: x: 2, y: 2, z: 4, core: 2. Of those that a mesh axis runs over, the one named last changes fastest.
Arguments:
- hot_ids: int32 [65536], P(('rep', 'shard')), may hold values from 0 to 8191
- hot_grads: bfloat16 [65536, 128], P(('rep', 'shard')), may hold values from -6 to 6
- hot_rows: float32 [8192, 128], replicated, may hold values from -6 to 6
- hot_accum: float32 [8192], replicated, may hold values from 0.5 to 4
- cold_counts: int32 [32, 32], P(('rep', 'shard')), may hold values from 1 to 16, as said below
- cold_slots: int32 [32, 32, 16], P(('rep', 'shard')), may hold values from 0 to 8191
- cold_grads: bfloat16 [32, 32, 16, 128], P(('rep', 'shard')), may hold values from -6 to 6
- cold_rows: float32 [262144, 128], P(('rep', 'shard')), may hold values from -6 to 6
- cold_accum: float32 [262144], P(('rep', 'shard')), may hold values from 0.5 to 4
Outputs:
- new_hot_rows: float32 [8192, 128], replicated
- new_hot_accum: float32 [8192], replicated
- new_cold_rows: float32 [262144, 128], P(('rep', 'shard'))
- new_cold_accum: float32 [262144], P(('rep', 'shard'))
The draws below stay inside these ranges and needn't reach their ends.
Inputs may be any that keep to these rules, and one draw needn't show every extreme that they name: `cold_counts`: every entry is at least 1 and at most 16; in every draw some owner receives 16 live slots from every sender.
All inputs are finite; a program needn't handle non-finite values.
Results may differ from the reference program's by a relative error of at most 0.0003.
Values may be sent and summed in bfloat16 or wider, within the bound.
A program may use at most 128 MiB of HBM per device.

```python
import math
import jax
import jax.numpy as jnp
import numpy as np
from jax import lax

D = 128
HOT = 8192
COLD_DEV = 8192
CAP = 16
OWNERS = 32
COLD = 262144
LOOKUPS = 65536


def draw_cold_counts(key, part):
    level_key = jax.random.fold_in(key, 11)
    draw_key = jax.random.fold_in(key, 12)
    full_key = jax.random.fold_in(key, 13)
    load_level = jax.random.randint(level_key, (OWNERS,), 1, 5)
    raw_draw = jax.random.randint(draw_key, (OWNERS, OWNERS), 0, CAP)
    counts = jnp.minimum(CAP, 1 + raw_draw * load_level[None, :] // 4)
    full_owner = jax.random.randint(full_key, (), 0, OWNERS)
    counts = jnp.where(jnp.arange(OWNERS)[None, :] == full_owner, CAP, counts)
    return counts.astype(jnp.int32)


def set_ends(array, rng, least, high):
    spot = [jax.random.randint(jax.random.fold_in(rng, axis), (), 0, length) for axis, length in enumerate(array.shape)]
    main_axis = array.shape.index(max(array.shape))
    neighbour = spot[:main_axis] + [(spot[main_axis] + 1) % array.shape[main_axis]] + spot[main_axis + 1:]
    return array.at[tuple(spot)].set(least).at[tuple(neighbour)].set(high)


def level_of(own_key, extent, cuts, least, top_value):
    def one(dim, shards_of):
        heights = jax.random.uniform(jax.random.fold_in(jax.random.fold_in(own_key, 6), dim), (shards_of,), jnp.float32, least / len(cuts), top_value / len(cuts))
        return jnp.repeat(jnp.exp(heights), extent[dim] // shards_of).reshape((-1,) + (1,) * (len(extent) - dim - 1))

    factor_of = one(*cuts[0])
    for cut in cuts[1:]:
        factor_of = factor_of * one(*cut)
    return factor_of


def rank_table(number_of, slope):
    portions = [(1 << 20) // math.isqrt(grade ** slope) + 1 for grade in range(1, number_of + 1)]
    spread = 1 + sum(portions) // (1 << 30)
    return np.cumsum(np.array([max(1, weight // spread) for weight in portions]))


def ranked_ids(key, shape, number_of, lean):
    table = rank_table(number_of, lean)
    pick = jax.random.randint(jax.random.fold_in(key, 1), shape, 0, int(table[number_of - 1]))
    grade = jnp.searchsorted(jnp.asarray(table, jnp.int32), pick, side="right")
    return jax.random.permutation(jax.random.fold_in(key, 2), number_of)[grade].astype(jnp.int32)


def noise(rng, extent, deviation, reach, shards=(), kind=jnp.bfloat16):
    result = jax.random.normal(rng, extent, jnp.float32) * deviation
    if len(shards) > 0:
        result = level_of(rng, extent, shards, -0.22, 0.18) * result
    return jnp.clip(result, min=-reach, max=reach).astype(kind)


def setup_inputs(seed: int = 0) -> dict:
    seeds = jax.random.split(jax.random.key(seed), 10)
    return {
        "hot_ids": set_ends(ranked_ids(seeds[0], (LOOKUPS,), HOT, 2), jax.random.fold_in(seeds[0], 3), 0, HOT - 1).astype(jnp.int32),
        "hot_grads": noise(seeds[1], (LOOKUPS, D), 1.0, 6.0, ((0, 32),)),
        "hot_rows": noise(seeds[2], (HOT, D), 1.0, 6.0, (), jnp.float32),
        "hot_accum": jnp.clip(jnp.exp(jax.random.uniform(seeds[3], (HOT,), jnp.float32, math.log(0.5), math.log(4.0))), 0.5, 4.0),
        "cold_counts": draw_cold_counts(jax.random.fold_in(seeds[9], 71), 0),
        "cold_slots": set_ends(jax.random.randint(seeds[5], (OWNERS, OWNERS, CAP), 0, COLD_DEV), jax.random.fold_in(seeds[5], 1), 0, COLD_DEV - 1).astype(jnp.int32),
        "cold_grads": noise(seeds[6], (OWNERS, OWNERS, CAP, D), 1.0, 6.0, ((0, 32),)),
        "cold_rows": noise(seeds[7], (COLD, D), 1.0, 6.0, ((0, 32),), jnp.float32),
        "cold_accum": jnp.clip(jnp.exp(math.log(4.0) - 2.0794415 * jax.random.uniform(seeds[8], (COLD,), jnp.float32) ** level_of(seeds[8], (COLD,), ((0, 32),), -0.2, 0.2)), 0.5, 4.0),
    }


learn_rate = 0.5

def adagrad(table_rows, accum_rows, gradient):
    accum_new = accum_rows + lax.optimization_barrier(jnp.mean(gradient * gradient, axis=1))
    return (table_rows - learn_rate * gradient / jnp.sqrt(accum_new)[:, None], accum_new)

def reference(hot_ids, hot_grads, hot_rows, hot_accum, cold_counts, cold_slots, cold_grads, cold_rows, cold_accum):
    hot_sum = jax.ops.segment_sum(hot_grads.astype(jnp.float32), hot_ids, num_segments=HOT)
    new_hot_rows, new_hot_accum = adagrad(hot_rows, hot_accum, hot_sum)
    slot_index = jnp.arange(CAP, dtype=jnp.int32)
    live_mask = slot_index[None, None, :] < cold_counts[:, :, None]
    owners_col = jnp.arange(OWNERS, dtype=jnp.int32)[None, :, None]
    target = (owners_col * COLD_DEV + cold_slots).astype(jnp.int32)
    masked_terms = jnp.where(live_mask[..., None], cold_grads.astype(jnp.float32), 0.0)
    cold_sum = jax.ops.segment_sum(masked_terms.reshape(-1, D), target.reshape(-1), num_segments=COLD)
    new_cold_rows, new_cold_accum = adagrad(cold_rows, cold_accum, cold_sum)
    return (new_hot_rows, new_hot_accum, new_cold_rows, new_cold_accum)
```

```python
import functools

import jax
import jax.numpy as jnp
from jax import lax
from jax.experimental import pallas as pl
from jax.experimental.pallas import tpu as pltpu
from jax.sharding import PartitionSpec as P

learn_rate = 0.5
LANES = 128
UNITS = 8
TILE = 256
BOTH = ("rep", "shard")


def adagrad(rows, accum_row, grad):
    m = rows.shape[0]
    diag = lax.broadcasted_iota(jnp.int32, (m, LANES), 0) == lax.broadcasted_iota(
        jnp.int32, (m, LANES), 1
    )
    square = jnp.sum(grad * grad, axis=1, keepdims=True) * (1.0 / grad.shape[1])
    accum = jnp.sum(jnp.where(diag, accum_row, 0.0), axis=1, keepdims=True)
    accum_new = accum + square
    rows_new = rows - grad * (learn_rate / jnp.sqrt(accum_new))
    accum_new_row = jnp.sum(jnp.where(diag, accum_new, 0.0), axis=0, keepdims=True)
    return rows_new, accum_new_row


def onehot_dot(ids, base, rows, grads):
    lookups = ids.shape[1]
    row = lax.broadcasted_iota(jnp.int32, (rows, lookups), 0)
    hit = jnp.where(row == ids - base, 1.0, 0.0).astype(jnp.bfloat16)
    return jnp.dot(hit, grads, preferred_element_type=jnp.float32)


def log2(n):
    return n.bit_length() - 1


def unit_orders(rep_bits, depth_bits):
    across = [("rep", b) for b in range(rep_bits)]
    along = [("depth", b) for b in range(depth_bits)]
    back = across[::-1]
    first = [across + along, back + along]
    third = [along[:1] + across + along[1:], along[:1] + back + along[1:]]
    kinds = [first[0], first[1], third[0], first[0], first[1], third[1], first[0], first[1]]
    return [kinds[u % len(kinds)] for u in range(UNITS)]


def plan(steps):
    stages = 2 * steps + 3
    events = []
    for u in range(UNITS):
        for s in range(stages):
            events.append((2.0 * u + 3.0 * s, s, u))
    for c in range(UNITS):
        events.append((14.0 + 2.0 * c, -1, c))
    return [(s, u) for _, s, u in sorted(events)]


def kernel(
    reps, shards,
    ids, grads, hot_rows, hot_accum, slots, counts, cold_grads, cold_rows, cold_accum,
    hot_out, hot_accum_out, cold_out, cold_accum_out,
    ids_buf, grads_buf, acc, rs_buf, sums, hot_acc_buf, cold_acc_buf, slots_buf, counts_buf,
    cold_own, cold_ids, cids_buf, cgrads_buf,
    load_sem, raw_send, raw_recv, rs_send, rs_recv, ag_send, ag_recv, cross_send, cross_recv,
    cold_send, cold_recv,
):
    total = reps * shards
    depth = shards // 2
    groups = reps * depth
    steps = log2(groups)
    unit_rows = acc.shape[1]
    own = unit_rows // groups
    blocks = unit_rows // LANES
    rep, shard = lax.axis_index("rep"), lax.axis_index("shard")
    z, core = shard // 2, shard % 2
    me = rep * shards + shard
    partner = {"rep": rep, "shard": z * 2 + 1 - core}
    orders = unit_orders(log2(reps), log2(depth))

    def bit_of(dim):
        kind, b = dim
        return ((rep if kind == "rep" else z) // (1 << b)) % 2

    def neighbour(dim):
        kind, b = dim
        move = (1 << b) * (1 - 2 * bit_of(dim))
        if kind == "rep":
            return {"rep": rep + move, "shard": shard}
        return {"rep": rep, "shard": (z + move) * 2 + core}

    def remote(src, dst, s_sem, r_sem, device):
        return pltpu.make_async_remote_copy(
            src_ref=src, dst_ref=dst, send_sem=s_sem, recv_sem=r_sem,
            device_id=device, device_id_type=pl.DeviceIdType.MESH,
        )

    loads = [
        pltpu.make_async_copy(src, dst, load_sem.at[k])
        for k, (src, dst) in enumerate((
            (ids, ids_buf.at[0]), (grads, grads_buf.at[0]), (slots, slots_buf), (counts, counts_buf),
            (cold_grads, cold_own), (cold_grads.at[me], cgrads_buf.at[me]), (cold_rows, cold_out),
            (hot_rows, hot_out), (hot_accum, hot_acc_buf), (cold_accum, cold_acc_buf),
        ))
    ]
    for copy in loads:
        copy.start()

    barrier = pltpu.get_barrier_semaphore()

    @pl.loop(1, total)
    def _(d):
        p = (me + d) % total
        pl.semaphore_signal(
            barrier, inc=1, device_id={"rep": p // shards, "shard": p % shards},
            device_id_type=pl.DeviceIdType.MESH,
        )

    tiles = unit_rows // TILE

    def partial_sum(src, tile):
        base = core * (UNITS * unit_rows) + tile * TILE
        return onehot_dot(ids_buf[src], base, TILE, grads_buf[src])

    def own_part(first, last):
        @pl.loop(first * tiles, last * tiles)
        def _(t):
            acc[t // tiles, pl.ds(pl.multiple_of((t % tiles) * TILE, TILE), TILE)] = partial_sum(0, t)

    def partner_part(u):
        @pl.loop(0, tiles)
        def _(t):
            acc[u, pl.ds(pl.multiple_of(t * TILE, TILE), TILE)] += partial_sum(1, u * tiles + t)

    for copy in loads[:2]:
        copy.wait()
    own_part(0, UNITS // 2)

    capacity = slots_buf.shape[0]
    group = LANES // capacity
    for copy in loads[2:6]:
        copy.wait()
    slot = lax.broadcasted_iota(jnp.int32, (capacity, total), 0)
    live = jnp.where(slot < counts_buf[...], slots_buf[...] + 1, 0)
    lane_group = lax.broadcasted_iota(jnp.int32, (LANES, total), 0) // capacity
    spread = jnp.where(lane_group == me % group, jnp.concatenate([live] * group, axis=0), 0)
    cold_ids[...] = jnp.transpose(spread).reshape(total, 1, LANES)
    cids_buf[me] = cold_ids[me]

    pl.semaphore_wait(barrier, total - 1)

    raw = [
        remote(buf.at[0], buf.at[1], raw_send.at[k], raw_recv.at[k], partner)
        for k, buf in enumerate((ids_buf, grads_buf))
    ]
    for copy in raw:
        copy.start()

    @pl.loop(1, total)
    def _(d):
        p = (me + d) % total
        device = {"rep": p // shards, "shard": p % shards}
        remote(cold_ids.at[p], cids_buf.at[me], cold_send.at[0], cold_recv.at[0], device).start()
        remote(cold_own.at[p], cgrads_buf.at[me], cold_send.at[1], cold_recv.at[1], device).start()

    own_part(UNITS // 2, UNITS)
    for copy in raw:
        copy.wait_recv()

    ranges = []
    for order in orders:
        low, size, found = 0, groups, []
        for dim in order:
            size //= 2
            bit = bit_of(dim)
            mine = low + size * bit
            found.append((mine, low + size * (1 - bit), size))
            low = mine
        ranges.append(found)

    def span(start, size):
        return pl.ds(pl.multiple_of(start * own, own), size * own)

    def rs_copy(u, s):
        _, other, size = ranges[u][s]
        k = u * steps + s
        return remote(
            acc.at[u, span(other, size)], rs_buf.at[u, pl.ds(unit_rows - 2 * size * own, size * own)],
            rs_send.at[k], rs_recv.at[k], neighbour(orders[u][s]),
        )

    def block_of(u):
        return core * UNITS + u

    def ag_copy(u, s, arriving=False):
        mine, other, size = ranges[u][s]
        k = u * steps + s
        part = sums.at[block_of(u), span(other if arriving else mine, size)]
        return remote(part, part, ag_send.at[k], ag_recv.at[k], neighbour(orders[u][s]))

    def cross_copy(u, half, arriving=False):
        mine, other, size = ranges[u][0]
        block = (1 - core) * UNITS + u if arriving else block_of(u)
        part = sums.at[block, span((mine, other)[half], size)]
        k = 2 * u + half
        return remote(part, part, cross_send.at[k], cross_recv.at[k], partner)

    def update(block):
        @pl.loop(0, blocks)
        def _(j):
            at = block * blocks + j
            grad = sums[block, pl.ds(pl.multiple_of(j * LANES, LANES), LANES)]
            new_rows, new_accum = adagrad(hot_out[at], hot_acc_buf[at], grad)
            hot_out[at] = new_rows
            hot_accum_out[at] = new_accum

    sends = []

    def send(copy):
        copy.start()
        sends.append(copy)

    cold_steps = cold_out.shape[0] // TILE
    per_tile = TILE // LANES

    def cold_part(c):
        if c == 0:
            for copy in loads[6:]:
                copy.wait()
            for k, buf in enumerate((cids_buf, cgrads_buf)):
                part = buf.at[pl.ds(0, total - 1)]
                pltpu.make_async_copy(part, part, cold_recv.at[k]).wait()
        row = jnp.concatenate(
            [jnp.sum(cids_buf[g * group:(g + 1) * group], axis=0) for g in range(total // group)],
            axis=1,
        ) - 1

        @pl.loop(c * cold_steps // UNITS, (c + 1) * cold_steps // UNITS)
        def _(b):
            terms = cgrads_buf[...].reshape(total * capacity, LANES)
            grad = onehot_dot(row, b * TILE, TILE, terms)
            for s in range(per_tile):
                at = pl.ds(pl.multiple_of(b * TILE + s * LANES, LANES), LANES)
                new_rows, new_accum = adagrad(
                    cold_out[at], cold_acc_buf[per_tile * b + s], grad[s * LANES:(s + 1) * LANES]
                )
                cold_out[at] = new_rows
                cold_accum_out[per_tile * b + s] = new_accum

    def stage(s, u):
        if s == 0:
            partner_part(u)
            send(rs_copy(u, 0))
        elif s <= steps:
            rs_copy(u, s - 1).wait_recv()
            mine, _, size = ranges[u][s - 1]
            at = span(mine, size)
            arrived = rs_buf[u, pl.ds(unit_rows - 2 * size * own, size * own)]
            if s < steps:
                acc[u, at] += arrived
                send(rs_copy(u, s))
            else:
                sums[block_of(u), at] = acc[u, at] + arrived
                send(ag_copy(u, steps - 1))
        elif s < 2 * steps:
            ag_copy(u, 2 * steps - s, True).wait_recv()
            send(ag_copy(u, 2 * steps - 1 - s))
            if s == 2 * steps - 1:
                send(cross_copy(u, 0))
        elif s == 2 * steps:
            ag_copy(u, 0, True).wait_recv()
            send(cross_copy(u, 1))
        elif s == 2 * steps + 1:
            update(block_of(u))
        else:
            for half in range(2):
                cross_copy(u, half, True).wait_recv()
            update((1 - core) * UNITS + u)

    for s, u in plan(steps):
        if s < 0:
            cold_part(u)
        else:
            stage(s, u)

    for copy in raw + sends:
        copy.wait_send()
    for k, buf in enumerate((cold_ids, cold_own)):
        part = buf.at[pl.ds(0, total - 1)]
        pltpu.make_async_copy(part, part, cold_send.at[k]).wait()


def flush(hot, hot_accum, cold, cold_accum, hot_out, hot_accum_out, cold_out, cold_accum_out, sem):
    copies = [
        pltpu.make_async_copy(src, dst, sem.at[k])
        for k, (src, dst) in enumerate((
            (hot, hot_out), (cold, cold_out), (hot_accum, hot_accum_out), (cold_accum, cold_accum_out),
        ))
    ]
    for copy in copies:
        copy.start()
    for copy in copies:
        copy.wait()


def local(
    hot_ids, hot_grads, hot_rows, hot_accum, cold_counts, cold_slots, cold_grads, cold_rows, cold_accum
):
    reps, shards = lax.axis_size("rep"), lax.axis_size("shard")
    total, groups = reps * shards, reps * shards // 2
    assert reps & (reps - 1) == 0 and shards & (shards - 1) == 0
    steps = log2(groups)
    hot_count, width = hot_rows.shape
    lookups = hot_ids.shape[0]
    unit_rows = hot_count // (2 * UNITS)
    cold_count = cold_rows.shape[0]
    capacity = cold_slots.shape[2]
    assert width == LANES and LANES % capacity == 0
    assert unit_rows % (8 * groups) == 0 and unit_rows % TILE == 0
    hot_blocks, cold_blocks = hot_count // LANES, cold_count // LANES

    f32, i32, bf16 = jnp.float32, jnp.int32, jnp.bfloat16
    vmem, anywhere = pl.BlockSpec(memory_space=pltpu.VMEM), pl.BlockSpec(memory_space=pl.ANY)
    dma = pltpu.SemaphoreType.DMA
    results = pl.pallas_call(
        functools.partial(kernel, reps, shards),
        out_shape=(
            pltpu.VMEM((hot_blocks, LANES, LANES), f32),
            pltpu.VMEM((hot_blocks, 1, LANES), f32),
            pltpu.VMEM((cold_count, LANES), f32),
            pltpu.VMEM((cold_blocks, 1, LANES), f32),
        ),
        in_specs=[anywhere] * 9,
        out_specs=(vmem,) * 4,
        scratch_shapes=[
            pltpu.VMEM((2, 1, lookups), i32),
            pltpu.VMEM((2, lookups, LANES), bf16),
            pltpu.VMEM((UNITS, unit_rows, LANES), f32),
            pltpu.VMEM((UNITS, unit_rows, LANES), f32),
            pltpu.VMEM((2 * UNITS, unit_rows, LANES), f32),
            pltpu.VMEM((hot_blocks, 1, LANES), f32),
            pltpu.VMEM((cold_blocks, 1, LANES), f32),
            pltpu.VMEM((capacity, total), i32),
            pltpu.VMEM((1, total), i32),
            pltpu.VMEM((total, capacity, LANES), bf16),
            pltpu.VMEM((total, 1, LANES), i32),
            pltpu.VMEM((total, 1, LANES), i32),
            pltpu.VMEM((total, capacity, LANES), bf16),
            dma((10,)), dma((2,)), dma((2,)),
            dma((UNITS * steps,)), dma((UNITS * steps,)), dma((UNITS * steps,)), dma((UNITS * steps,)),
            dma((2 * UNITS,)), dma((2 * UNITS,)), dma((2,)), dma((2,)),
        ],
        compiler_params=pltpu.CompilerParams(
            collective_id=0, has_side_effects=True, vmem_limit_bytes=40 * 1024 * 1024
        ),
    )(
        hot_ids.reshape(1, lookups),
        hot_grads,
        hot_rows.reshape(hot_blocks, LANES, LANES),
        hot_accum.reshape(hot_blocks, 1, LANES),
        cold_slots.reshape(total, capacity).T,
        cold_counts,
        cold_grads.reshape(total, capacity, LANES),
        cold_rows,
        cold_accum.reshape(cold_blocks, 1, LANES),
    )
    results = [pltpu.with_memory_space_constraint(x, pltpu.VMEM) for x in results]
    hot_new, hot_accum_new, cold_new, cold_accum_new = pl.pallas_call(
        flush,
        out_shape=tuple(jax.ShapeDtypeStruct(x.shape, f32) for x in results),
        in_specs=[vmem] * 4,
        out_specs=(anywhere,) * 4,
        scratch_shapes=[dma((4,))],
        compiler_params=pltpu.CompilerParams(vmem_limit_bytes=16 * 1024 * 1024),
    )(*results)
    return (
        hot_new.reshape(hot_count, LANES),
        hot_accum_new.reshape(hot_count),
        cold_new,
        cold_accum_new.reshape(cold_count),
    )


def solution(mesh):
    placed = (
        P(BOTH), P(BOTH, None), P(), P(), P(BOTH, None), P(BOTH, None, None),
        P(BOTH, None, None, None), P(BOTH, None), P(BOTH),
    )
    return jax.shard_map(
        local,
        mesh=mesh,
        in_specs=placed,
        out_specs=(P(), P(), P(BOTH, None), P(BOTH)),
        check_vma=False,
    )
```
